32 devices in a mesh: grp: 4 (over y, x), dev: 8 (over z, core).
Axes of the slice: x: 2, y: 2, z: 4, core: 2. Of those that a mesh axis runs over, the one named last changes fastest.
Arguments:
- obs_coord: float32 [3, 131072], P(None, ('grp', 'dev')), may hold values from -1 to 1
- obs_resid: float32 [131072], P(('grp', 'dev')), may hold values from -6 to 6
- obs_weight: float32 [131072], P(('grp', 'dev')), may hold values from 0.5 to 2
- obs_dest: int32 [131072], P(('grp', 'dev')), may hold values from 0 to 7, as said below
- obs_send_slot: int32 [131072], P(('grp', 'dev')), may hold values from 0 to 1023, as said below
- obs_elem: int32 [131072], P(('grp', 'dev')), may hold values from 0 to 255, as said below
- obs_slot: int32 [131072], P(('grp', 'dev')), may hold values from 0 to 31, as said below
Outputs:
- nodal: float32 [16, 64, 8, 512], P('grp', 'dev')
- total_cost: float32 [], replicated
The draws below stay inside these ranges and needn't reach their ends.
Inputs may be any that keep to these rules, and one draw needn't show every extreme that they name: `obs_dest`: from the rows of one device, at most 1024 observations go to any one destination; in every group one destination receives exactly 1024 from every device of the group. `obs_send_slot`: distinct among the rows of one device with the same obs_dest. `obs_elem`: together with obs_slot distinct among all observations of a group with the same obs_dest. `obs_slot`: on every destination some element uses all 32 slots.
All inputs are finite; a program needn't handle non-finite values.
Results may differ from the reference program's by a relative error of at most 0.00017.
Values sent between devices are 32-bit elements; how exact they have to be, the bound alone decides.
A program may use at most 64 MiB of HBM per device.

```python
import math
import jax
import jax.numpy as jnp
from jax import lax

OBS_DEV = 4096
EX = 4
EY = 8
EZ = 8
ELEM_DEV = 256
CAP = 1024
SLOTS = 32
TOTAL_OBS = 131072
NEX = 16
NEY = 64
N_GRP = 4
N_DEV = 8


def layout(key):
    peer_count = 2 * OBS_DEV // CAP
    group_count = TOTAL_OBS // (OBS_DEV * peer_count)
    cell_count = ELEM_DEV * SLOTS
    key_a, key_b, key_c, key_d, key_e = jax.random.split(key, 5)
    columns = jnp.arange(cell_count, dtype=jnp.int32)
    wanted = columns // CAP
    favored = jax.random.randint(key_a, (group_count, 1, 1), 0, peer_count, dtype=jnp.int32)
    jitter = jax.random.randint(key_b, (group_count, peer_count, cell_count), 1, 32768, dtype=jnp.int32)
    ranking = jnp.where(wanted[None, None, :] == favored, 0, jitter) * cell_count + columns
    picked = jnp.argsort(ranking, axis=-1)[:, :, :OBS_DEV].astype(jnp.int32)
    target = wanted[picked]
    row_ids = jnp.arange(OBS_DEV, dtype=jnp.int32)
    shuffle_keys = jax.random.randint(key_c, (group_count, peer_count, OBS_DEV), 0, 32768, dtype=jnp.int32) * OBS_DEV + row_ids
    mixing = jnp.argsort(shuffle_keys, axis=-1).astype(jnp.int32)
    target = jnp.take_along_axis(target, mixing, axis=-1)
    sorter = jnp.argsort(target, axis=-1, stable=True).astype(jnp.int32)
    sorted_target = jnp.take_along_axis(target, sorter, axis=-1)
    steps_row = jnp.broadcast_to(row_ids, sorted_target.shape)
    change = jnp.concatenate([jnp.ones((group_count, peer_count, 1), bool), sorted_target[:, :, 1:] != sorted_target[:, :, :-1]], axis=-1)
    starts = lax.cummax(jnp.where(change, steps_row, 0), axis=2)
    ranks_sorted = steps_row - starts
    inverse = jnp.argsort(sorter, axis=-1).astype(jnp.int32)
    send_slot = jnp.take_along_axis(ranks_sorted, inverse, axis=-1)
    owner = jnp.arange(group_count * peer_count, dtype=jnp.int32).reshape(group_count, peer_count, 1)
    segment = (owner * peer_count + target).reshape(-1)
    counts = jax.ops.segment_sum(jnp.ones_like(segment), segment, num_segments=group_count * peer_count * peer_count)
    counts = counts.reshape(group_count, peer_count, peer_count)
    earlier = jnp.cumsum(counts, axis=1) - counts
    arrival = jnp.take_along_axis(earlier, target, axis=2) + send_slot
    favored_elem = jax.random.randint(key_d, (group_count, peer_count, 1), 0, ELEM_DEV, dtype=jnp.int32)
    jitter_two = jax.random.randint(key_e, (group_count, peer_count, cell_count), 1, 32768, dtype=jnp.int32)
    ranking_two = jnp.where((columns // SLOTS)[None, None, :] == favored_elem, 0, jitter_two) * cell_count + columns
    table = jnp.argsort(ranking_two, axis=-1).astype(jnp.int32)
    group_ids = jnp.arange(group_count, dtype=jnp.int32).reshape(group_count, 1, 1)
    flat_index = ((group_ids * peer_count + target) * cell_count + arrival).reshape(-1)
    chosen = table.reshape(-1)[flat_index]
    return (target.reshape(-1).astype(jnp.int32), send_slot.reshape(-1).astype(jnp.int32), (chosen // SLOTS).astype(jnp.int32), (chosen % SLOTS).astype(jnp.int32))


def draw_obs_dest(key, part):
    return layout(jax.random.fold_in(key, 11))[0]


def draw_obs_send_slot(key, part):
    return layout(jax.random.fold_in(key, 11))[1]


def draw_obs_elem(key, part):
    return layout(jax.random.fold_in(key, 11))[2]


def draw_obs_slot(key, part):
    return layout(jax.random.fold_in(key, 11))[3]


def block_levels(stream_key, dims, pieces, smallest, top_value):
    level, own = 1.0, jax.random.fold_in(stream_key, 6)
    for dim, parts in pieces:
        draws = jnp.exp(jax.random.uniform(jax.random.fold_in(own, dim), (parts,), jnp.float32, smallest / len(pieces), top_value / len(pieces)))
        level = level * jnp.repeat(draws, dims[dim] // parts).reshape([-1 if axis == dim else 1 for axis in range(len(dims))])
    return level


def gaussian(stream_key, shape, width, reach, cuts=(), kind=jnp.bfloat16):
    loudness = block_levels(stream_key, shape, cuts, -0.22, 0.18) if cuts else 1.0
    array = jax.random.normal(stream_key, shape, jnp.float32) * width * loudness
    return jnp.minimum(jnp.maximum(array, -reach), reach).astype(kind)


def setup_inputs(seed: int = 0) -> dict:
    keys = jax.random.split(jax.random.key(seed), 8)
    obs_coord = jnp.clip(jax.random.uniform(keys[0], (3, TOTAL_OBS), jnp.float32, -1.0, 1.0) * block_levels(keys[0], (3, TOTAL_OBS), ((1, 32),), -0.4, 0.0), -1.0, 1.0)
    obs_resid = gaussian(keys[1], (TOTAL_OBS,), 1.0, 6.0, ((0, 32),), jnp.float32)
    obs_weight = jnp.clip(jnp.exp(math.log(2.0) - 1.3862944 * jax.random.uniform(keys[2], (TOTAL_OBS,), jnp.float32) ** block_levels(keys[2], (TOTAL_OBS,), ((0, 32),), -0.2, 0.2)), 0.5, 2.0)
    obs_dest = draw_obs_dest(jax.random.fold_in(keys[7], 71), 0)
    obs_send_slot = draw_obs_send_slot(jax.random.fold_in(keys[7], 71), 0)
    obs_elem = draw_obs_elem(jax.random.fold_in(keys[7], 71), 0)
    obs_slot = draw_obs_slot(jax.random.fold_in(keys[7], 71), 0)
    return {"obs_coord": obs_coord, "obs_resid": obs_resid, "obs_weight": obs_weight, "obs_dest": obs_dest, "obs_send_slot": obs_send_slot, "obs_elem": obs_elem, "obs_slot": obs_slot}


def basis_values(position):
    anchors = [-math.cos(math.pi * k / 7) for k in range(8)]
    basis = []
    for node_i in range(8):
        factor = jnp.ones_like(position)
        for node_m in range(8):
            if node_m != node_i:
                factor = factor * ((position - anchors[node_m]) / (anchors[node_i] - anchors[node_m]))
        basis.append(factor)
    return jnp.stack(basis)


def contract(first_w, second_w, third_w):
    outer = (first_w[:, None, :] * second_w[None, :, :]).reshape(64, ELEM_DEV, SLOTS)
    third = third_w.reshape(8, ELEM_DEV, SLOTS)
    mixed = jnp.einsum("aes,kes->eak", outer, third, precision=lax.Precision.HIGHEST)
    return mixed.reshape(ELEM_DEV, 512)


def combine(field, elem_dim, node_dim, from_low, from_high):
    count = field.shape[elem_dim]
    low_plane = lax.slice_in_dim(field, 0, 1, axis=node_dim)
    high_plane = lax.slice_in_dim(field, 7, 8, axis=node_dim)
    after = jnp.concatenate([lax.slice_in_dim(low_plane, 1, count, axis=elem_dim), from_high], axis=elem_dim)
    before = jnp.concatenate([from_low, lax.slice_in_dim(high_plane, 0, count - 1, axis=elem_dim)], axis=elem_dim)
    middle = lax.slice_in_dim(field, 1, 7, axis=node_dim)
    return jnp.concatenate([low_plane + before, middle, high_plane + after], axis=node_dim)


def block_nodes(block):
    first_w = basis_values(block[0]) * block[3]
    return contract(first_w, basis_values(block[1]), basis_values(block[2]))


def reference(obs_coord, obs_resid, obs_weight, obs_dest, obs_send_slot, obs_elem, obs_slot):
    forcing = obs_weight * obs_resid
    total_cost = 0.5 * jnp.sum(forcing * obs_resid)
    cell_count = ELEM_DEV * SLOTS
    device_count = N_GRP * N_DEV
    source = jnp.arange(TOTAL_OBS, dtype=jnp.int32) // OBS_DEV
    group_index = source // N_DEV
    device = group_index * N_DEV + obs_dest
    position = device * cell_count + obs_elem * SLOTS + obs_slot
    values = jnp.concatenate([obs_coord, forcing[None, :]], axis=0)
    packed = jnp.zeros((4, device_count * cell_count), obs_coord.dtype).at[:, position].set(values)
    blocks = packed.reshape(4, device_count, cell_count).transpose(1, 0, 2)
    raw = lax.map(block_nodes, blocks)
    raw = raw.reshape(N_GRP, N_DEV, EX, EY, EZ, 512).transpose(0, 2, 1, 3, 4, 5)
    field = raw.reshape(NEX, NEY, EZ, 8, 8, 8)
    for elem_dim in range(3):
        node_dim = elem_dim + 3
        edge = lax.slice_in_dim(lax.slice_in_dim(field, 0, 1, axis=node_dim), 0, 1, axis=elem_dim)
        empty = jnp.zeros_like(edge)
        field = combine(field, elem_dim, node_dim, empty, empty)
    return field.reshape(NEX, NEY, EZ, 512), total_cost
```

```python
import functools
import math

import jax
import jax.numpy as jnp
from jax import lax
from jax.experimental import pallas as pl
from jax.experimental.pallas import tpu as pltpu
from jax.sharding import PartitionSpec as P

EX = 4
EY = 8
EZ = 8
ELEM_DEV = 256
LANES = 128
CHUNK = 1024
MESH = pl.DeviceIdType.MESH
F32 = jnp.float32
BF16 = jnp.bfloat16

ANCHORS = [-math.cos(math.pi * k / 7) for k in range(8)]
COEFS = [
    1.0 / math.prod(ANCHORS[a] - ANCHORS[m] for m in range(8) if m != a) for a in range(8)
]


def basis_values(t):
    factors = [t - p for p in ANCHORS]
    prefix = [None] * 8
    suffix = [None] * 8
    for k in range(1, 8):
        prefix[k] = factors[k - 1] if k == 1 else prefix[k - 1] * factors[k - 1]
    for k in range(6, -1, -1):
        suffix[k] = factors[k + 1] if k == 6 else suffix[k + 1] * factors[k + 1]
    basis = []
    for a in range(8):
        if a == 0:
            product = suffix[0]
        elif a == 7:
            product = prefix[7]
        else:
            product = prefix[a] * suffix[a]
        basis.append(product * COEFS[a])
    return basis


def dot_nt(left, right):
    return lax.dot_general(left, right, (((1,), (1,)), ((), ())), preferred_element_type=F32)


def split3(value):
    first = value.astype(BF16).astype(F32)
    rest = value - first
    second = rest.astype(BF16).astype(F32)
    return first, second, rest - second


def kernel(
    dev_count, grp_count, capacity,
    coord, resid, weight, dest, slot, elem,
    out, cost,
    acc, send, recv, cost_send, cost_recv, group_send, group_recv,
    third, outer, p_high, p_low, onehot, raw, a_send, a_recv, b_send, b_recv,
    send_sem, recv_sem, cost_send_sem, cost_recv_sem, group_send_sem, group_recv_sem,
    face_send_sem, face_recv_sem,
):
    g = lax.axis_index("grp")
    d = lax.axis_index("dev")
    row_count = resid.shape[1]
    row_total = 2 * row_count // LANES
    per_dest = capacity // LANES
    per_chunk = 8 // per_dest

    barrier = pltpu.get_barrier_semaphore()
    for j in range(1, dev_count):
        pl.semaphore_signal(
            barrier, inc=1, device_id=(g, lax.rem(d + j, dev_count)), device_id_type=MESH
        )
    for j in range(1, grp_count):
        pl.semaphore_signal(
            barrier, inc=1, device_id=(lax.rem(g + j, grp_count), d), device_id_type=MESH
        )

    acc[...] = jnp.zeros_like(acc)

    def pack(k, total):
        columns = pl.ds(pl.multiple_of(k * CHUNK, CHUNK), CHUNK)
        target = dest[:, columns] * capacity + slot[:, columns]
        high = jnp.broadcast_to(target // LANES, (row_total, CHUNK))
        low = jnp.broadcast_to(target % LANES, (LANES, CHUNK))
        row_hot = jnp.where(
            lax.broadcasted_iota(jnp.int32, (row_total, CHUNK), 0) == high, 1.0, 0.0
        ).astype(BF16)
        lane_hot = jnp.where(
            lax.broadcasted_iota(jnp.int32, (LANES, CHUNK), 0) == low, 1.0, 0.0
        ).astype(BF16)
        residual = resid[:, columns]
        forcing = weight[:, columns] * residual
        values = [coord[c : c + 1, columns] for c in range(3)] + [forcing]
        terms = [split3(value) for value in values]

        def spread(row):
            tile = jnp.broadcast_to(row, (16, CHUNK)).astype(BF16)
            return [row_hot[16 * i : 16 * i + 16] * tile for i in range(row_total // 16)]

        for t in range(3):
            pieces = []
            for channel in range(4):
                pieces += spread(terms[channel][t])
            if t == 0:
                pieces += spread(elem[:, columns].astype(F32))
            left = jnp.concatenate(pieces, axis=0)
            acc[0 : left.shape[0], :] += dot_nt(left, lane_hot)
        return total + forcing * residual

    total = lax.fori_loop(0, row_count // CHUNK, pack, jnp.zeros((1, CHUNK), F32))
    part = jnp.broadcast_to(0.5 * jnp.sum(total, axis=1, keepdims=True), (1, LANES))
    cost_send[...] = part
    for p in range(dev_count):
        for c in range(5):
            start = c * row_total + p * per_dest
            send[p, c * per_dest : (c + 1) * per_dest, :] = acc[start : start + per_dest, :]

    pl.semaphore_wait(barrier, dev_count - 1 + grp_count - 1)

    def data_copy(j):
        peer = lax.rem(d + j, dev_count)
        return pltpu.make_async_remote_copy(
            src_ref=send.at[peer], dst_ref=recv.at[j],
            send_sem=send_sem.at[j], recv_sem=recv_sem.at[j],
            device_id=(g, peer), device_id_type=MESH,
        )

    def cost_copy(j):
        return pltpu.make_async_remote_copy(
            src_ref=cost_send, dst_ref=cost_recv.at[j],
            send_sem=cost_send_sem.at[j], recv_sem=cost_recv_sem.at[j],
            device_id=(g, lax.rem(d + j, dev_count)), device_id_type=MESH,
        )

    def group_copy(j):
        return pltpu.make_async_remote_copy(
            src_ref=group_send, dst_ref=group_recv.at[j],
            send_sem=group_send_sem.at[j], recv_sem=group_recv_sem.at[j],
            device_id=(lax.rem(g + j, grp_count), d), device_id_type=MESH,
        )

    for j in range(1, dev_count):
        data_copy(j).start()
    for j in range(1, dev_count):
        cost_copy(j).start()
    recv[0] = send[d]

    raw[...] = jnp.zeros_like(raw)

    def element_sums(k, carry):
        for i in range(per_chunk):
            @pl.when(k * per_chunk + i > 0)
            def _():
                data_copy(k * per_chunk + i).wait_recv()

        def channel(c):
            rows = [
                recv[k * per_chunk + i, c * per_dest : (c + 1) * per_dest, :]
                for i in range(per_chunk)
            ]
            return rows[0] if per_chunk == 1 else jnp.concatenate(rows, axis=0)

        first_w = basis_values(channel(0))
        second_w = basis_values(channel(1))
        third_w = basis_values(channel(2))
        forcing = channel(3)
        owner = channel(4).astype(jnp.int32)
        for a in range(8):
            weighted = first_w[a] * forcing
            third[a] = third_w[a]
            for b in range(8):
                outer[a * 8 + b] = weighted * second_w[b]
        ids = lax.broadcasted_iota(jnp.int32, (ELEM_DEV, LANES), 0)
        for h in range(8):
            lanes = slice(h * LANES, (h + 1) * LANES)
            product = (outer[:, h : h + 1, :] * third[:, h, :][None]).reshape(512, LANES)
            rounded = product.astype(BF16)
            p_high[:, lanes] = rounded
            p_low[:, lanes] = (product - rounded.astype(F32)).astype(BF16)
            onehot[:, lanes] = jnp.where(
                ids == jnp.broadcast_to(owner[h : h + 1, :], (ELEM_DEV, LANES)), 1.0, 0.0
            ).astype(BF16)
        raw[...] += dot_nt(p_high[...], onehot[...]) + dot_nt(p_low[...], onehot[...])
        return carry

    lax.fori_loop(0, dev_count // per_chunk, element_sums, 0)

    group_cost = cost_send[...]
    for j in range(1, dev_count):
        cost_copy(j).wait_recv()
        group_cost = group_cost + cost_recv[j]
    group_send[...] = group_cost
    for j in range(1, grp_count):
        group_copy(j).start()

    lane = lax.broadcasted_iota(jnp.int32, (1, LANES), 1)
    lower_half = lane < 64
    block = raw[448:512, 128:256]
    a_send[0] = jnp.where(lower_half, pltpu.roll(block[0:32], 64, 1), block[32:64])
    block = raw[0:64, 0:128]
    a_send[1] = jnp.where(lower_half, block[0:32], pltpu.roll(block[32:64], 64, 1))

    def face_copy(i):
        step = 1 if i % 2 == 0 else -1
        if i < 2:
            source, sink = a_send.at[i], a_recv.at[i]
            target = (lax.rem(g + step + grp_count, grp_count), d)
        else:
            source, sink = b_send.at[i - 2], b_recv.at[i - 2]
            target = (g, lax.rem(d + step + dev_count, dev_count))
        return pltpu.make_async_remote_copy(
            src_ref=source, dst_ref=sink,
            send_sem=face_send_sem.at[i], recv_sem=face_recv_sem.at[i],
            device_id=target, device_id_type=MESH,
        )

    def start_faces(first, position, count):
        @pl.when(position < count - 1)
        def _():
            face_copy(first).start()

        @pl.when(position > 0)
        def _():
            face_copy(first + 1).start()

    def finish_faces(first, position, count, sink):
        @pl.when(position > 0)
        def _():
            face_copy(first).wait_recv()

        @pl.when(position == 0)
        def _():
            sink[0] = jnp.zeros_like(sink[0])

        @pl.when(position < count - 1)
        def _():
            face_copy(first + 1).wait_recv()

        @pl.when(position == count - 1)
        def _():
            sink[1] = jnp.zeros_like(sink[1])

    start_faces(0, g, grp_count)
    finish_faces(0, g, grp_count, a_recv)
    low, high = raw[0:64, :], raw[448:512, :]
    from_low, from_high = a_recv[0], a_recv[1]
    from_low = jnp.concatenate([from_low, pltpu.roll(from_low, 64, 1)], axis=0)
    from_high = jnp.concatenate([pltpu.roll(from_high, 64, 1), from_high], axis=0)
    high_rolled = [pltpu.roll(high[:, :128], 64, 1), pltpu.roll(high[:, 128:], 64, 1)]
    low_rolled = [pltpu.roll(low[:, :128], 64, 1), pltpu.roll(low[:, 128:], 64, 1)]
    raw[0:64, 0:128] = low[:, :128] + jnp.where(lower_half, from_low, high_rolled[0])
    raw[0:64, 128:256] = low[:, 128:] + jnp.where(lower_half, high_rolled[0], high_rolled[1])
    raw[448:512, 0:128] = high[:, :128] + jnp.where(lower_half, low_rolled[0], low_rolled[1])
    raw[448:512, 128:256] = high[:, 128:] + jnp.where(lower_half, low_rolled[1], from_high)

    ey = (lane // 8) % 8
    for half in range(2):
        columns = slice(half * LANES, (half + 1) * LANES)
        up = raw[56:64, columns]
        up = pltpu.roll(up, 72, 1)
        down = raw[0:8, columns]
        for a in range(1, 8):
            up = jnp.where(
                ey == a, pltpu.roll(raw[a * 64 + 56 : a * 64 + 64, columns], (a * 8 + 72) % 128, 1), up
            )
            down = jnp.where(
                ey == a, pltpu.roll(raw[a * 64 : a * 64 + 8, columns], a * 8, 1), down
            )
        b_send[0, half] = up
        b_send[1, half] = down
    start_faces(2, d, dev_count)
    finish_faces(2, d, dev_count, b_recv)
    for half in range(2):
        columns = slice(half * LANES, (half + 1) * LANES)
        from_low, from_high = b_recv[0, half], b_recv[1, half]
        for a in range(8):
            low_rows = slice(a * 64, a * 64 + 8)
            high_rows = slice(a * 64 + 56, a * 64 + 64)
            low, high = raw[low_rows, columns], raw[high_rows, columns]
            got_low = pltpu.roll(from_low, (128 - a * 8) % 128, 1)
            got_high = pltpu.roll(from_high, (56 - a * 8) % 128, 1)
            raw[low_rows, columns] = low + jnp.where(ey == 0, got_low, pltpu.roll(high, 8, 1))
            raw[high_rows, columns] = high + jnp.where(ey == 7, got_high, pltpu.roll(low, 120, 1))

    ez = lax.broadcasted_iota(jnp.int32, (1, 8, LANES), 2) % 8
    c = lax.broadcasted_iota(jnp.int32, (1, 8, LANES), 1)
    takes_low = (c == 0) & (ez > 0)
    takes_high = (c == 7) & (ez < 7)
    for half in range(2):
        for part in range(4):
            rows = slice(part * 128, (part + 1) * 128)
            field = raw[rows, half * LANES : (half + 1) * LANES].reshape(16, 8, LANES)
            below = pltpu.roll(pltpu.roll(field, 1, 2), 1, 1)
            above = pltpu.roll(pltpu.roll(field, 127, 2), 7, 1)
            field = field + jnp.where(takes_low, below, jnp.where(takes_high, above, 0.0))
            out[half * LANES : (half + 1) * LANES, rows] = field.reshape(128, LANES).T

    all_cost = group_send[...]
    for j in range(1, grp_count):
        group_copy(j).wait_recv()
        all_cost = all_cost + group_recv[j]
    cost[...] = all_cost

    for j in range(1, dev_count):
        data_copy(j).wait_send()
        cost_copy(j).wait_send()
    for j in range(1, grp_count):
        group_copy(j).wait_send()
    for first, position, count in ((0, g, grp_count), (2, d, dev_count)):
        @pl.when(position < count - 1)
        def _():
            face_copy(first).wait_send()

        @pl.when(position > 0)
        def _():
            face_copy(first + 1).wait_send()


def on_device(obs_coord, obs_resid, obs_weight, obs_dest, obs_send_slot, obs_elem, obs_slot):
    dev_count = lax.axis_size("dev")
    grp_count = lax.axis_size("grp")
    row_count = obs_resid.shape[0]
    capacity = 2 * row_count // dev_count
    per_dest = capacity // LANES
    vmem = pl.BlockSpec(memory_space=pltpu.VMEM)
    dma = pltpu.SemaphoreType.DMA
    rows = [x.reshape(1, row_count) for x in (obs_resid, obs_weight, obs_dest, obs_send_slot, obs_elem)]
    field, cost = pl.pallas_call(
        functools.partial(kernel, dev_count, grp_count, capacity),
        out_shape=(
            jax.ShapeDtypeStruct((ELEM_DEV, 512), F32),
            jax.ShapeDtypeStruct((1, LANES), F32),
        ),
        in_specs=[vmem] * 6,
        out_specs=(vmem, vmem),
        scratch_shapes=[
            pltpu.VMEM((5 * 2 * row_count // LANES, LANES), F32),
            pltpu.VMEM((dev_count, 5 * per_dest, LANES), F32),
            pltpu.VMEM((dev_count, 5 * per_dest, LANES), F32),
            pltpu.VMEM((1, LANES), F32),
            pltpu.VMEM((dev_count, 1, LANES), F32),
            pltpu.VMEM((1, LANES), F32),
            pltpu.VMEM((grp_count, 1, LANES), F32),
            pltpu.VMEM((8, 8, LANES), F32),
            pltpu.VMEM((64, 8, LANES), F32),
            pltpu.VMEM((512, CHUNK), BF16),
            pltpu.VMEM((512, CHUNK), BF16),
            pltpu.VMEM((ELEM_DEV, CHUNK), BF16),
            pltpu.VMEM((512, ELEM_DEV), F32),
            pltpu.VMEM((2, 32, LANES), F32),
            pltpu.VMEM((2, 32, LANES), F32),
            pltpu.VMEM((2, 2, 8, LANES), F32),
            pltpu.VMEM((2, 2, 8, LANES), F32),
            dma((dev_count,)),
            dma((dev_count,)),
            dma((dev_count,)),
            dma((dev_count,)),
            dma((grp_count,)),
            dma((grp_count,)),
            dma((4,)),
            dma((4,)),
        ],
        compiler_params=pltpu.CompilerParams(collective_id=0, has_side_effects=True),
    )(obs_coord, *rows)
    return field.reshape(EX, EY, EZ, 512), cost[0, 0]


def solution(mesh):
    placed = (
        P(None, ("grp", "dev")),
        P(("grp", "dev")),
        P(("grp", "dev")),
        P(("grp", "dev")),
        P(("grp", "dev")),
        P(("grp", "dev")),
        P(("grp", "dev")),
    )
    return jax.shard_map(
        on_device,
        mesh=mesh,
        in_specs=placed,
        out_specs=(P("grp", "dev", None, None), P()),
        check_vma=False,
    )
```

```python
import functools
import math

import jax
import jax.numpy as jnp
from jax import lax
from jax.experimental import pallas as pl
from jax.experimental.pallas import tpu as pltpu
from jax.sharding import PartitionSpec as P

EX = 4
EY = 8
EZ = 8
ELEM_DEV = 256
LANES = 128
CHUNK = 1024
MESH = pl.DeviceIdType.MESH
F32 = jnp.float32
BF16 = jnp.bfloat16

ANCHORS = [-math.cos(math.pi * k / 7) for k in range(8)]
COEFS = [
    1.0 / math.prod(ANCHORS[a] - ANCHORS[m] for m in range(8) if m != a) for a in range(8)
]


def basis_values(t):
    factors = [t - p for p in ANCHORS]
    prefix = [None] * 8
    suffix = [None] * 8
    for k in range(1, 8):
        prefix[k] = factors[k - 1] if k == 1 else prefix[k - 1] * factors[k - 1]
    for k in range(6, -1, -1):
        suffix[k] = factors[k + 1] if k == 6 else suffix[k + 1] * factors[k + 1]
    basis = []
    for a in range(8):
        if a == 0:
            product = suffix[0]
        elif a == 7:
            product = prefix[7]
        else:
            product = prefix[a] * suffix[a]
        basis.append(product * COEFS[a])
    return basis


def dot_nt(left, right):
    return lax.dot_general(left, right, (((1,), (1,)), ((), ())), preferred_element_type=F32)


def split3(value):
    first = value.astype(BF16).astype(F32)
    rest = value - first
    second = rest.astype(BF16).astype(F32)
    return first, second, rest - second


def kernel(
    dev_count, grp_count, capacity,
    coord_in, resid_in, weight_in, dest_in, slot_in, elem_in,
    out, cost,
    coord, resid, weight, dest, slot, elem, acc, send, recv, cost_send, cost_recv, group_send, group_recv,
    third, outer, p_high, p_low, onehot, raw, a_send, a_recv, b_send, b_recv,
    send_sem, recv_sem, cost_send_sem, cost_recv_sem, group_send_sem, group_recv_sem,
    face_send_sem, face_recv_sem, edge_recv, edge_send_sem, edge_recv_sem, load_sem,
):
    g = lax.axis_index("grp")
    d = lax.axis_index("dev")
    row_count = resid.shape[1]
    row_total = 2 * row_count // LANES
    per_dest = capacity // LANES
    per_chunk = 8 // per_dest

    def peer_of(k):
        peer, bit = 0, 1
        while bit < dev_count:
            peer = peer + lax.rem(d // bit + k // bit, 2) * bit
            bit *= 2
        return peer

    def wrapped(step_g, step_d):
        return (
            lax.rem(g + step_g + grp_count, grp_count),
            lax.rem(d + step_d + dev_count, dev_count),
        )

    barrier = pltpu.get_barrier_semaphore()
    partners = [(g, peer_of(k)) for k in range(1, dev_count)]
    partners += [wrapped(j, 0) for j in range(1, grp_count)]
    partners += [wrapped(i, j) for i in (-1, 1) for j in (-1, 1)]
    for partner in partners:
        pl.semaphore_signal(barrier, inc=1, device_id=partner, device_id_type=MESH)

    loads = [
        pltpu.make_async_copy(source, sink, load_sem.at[i])
        for i, (source, sink) in enumerate(
            zip(
                (dest_in, slot_in, resid_in, weight_in, coord_in, elem_in),
                (dest, slot, resid, weight, coord, elem),
            )
        )
    ]
    for load in loads:
        load.start()
    for load in loads:
        load.wait()

    acc[...] = jnp.zeros_like(acc)

    def pack(k, total):
        columns = pl.ds(pl.multiple_of(k * CHUNK, CHUNK), CHUNK)
        target = dest[:, columns] * capacity + slot[:, columns]
        high = jnp.broadcast_to(target // LANES, (row_total, CHUNK))
        low = jnp.broadcast_to(target % LANES, (LANES, CHUNK))
        row_hot = jnp.where(
            lax.broadcasted_iota(jnp.int32, (row_total, CHUNK), 0) == high, 1.0, 0.0
        ).astype(BF16)
        lane_hot = jnp.where(
            lax.broadcasted_iota(jnp.int32, (LANES, CHUNK), 0) == low, 1.0, 0.0
        ).astype(BF16)
        residual = resid[:, columns]
        forcing = weight[:, columns] * residual
        values = [coord[c : c + 1, columns] for c in range(3)] + [forcing]
        terms = [split3(value) for value in values]

        def spread(row):
            tile = jnp.broadcast_to(row, (16, CHUNK)).astype(BF16)
            return [row_hot[16 * i : 16 * i + 16] * tile for i in range(row_total // 16)]

        for t in range(3):
            pieces = []
            for channel in range(4):
                pieces += spread(terms[channel][t])
            if t == 0:
                pieces += spread(elem[:, columns].astype(F32))
            left = jnp.concatenate(pieces, axis=0)
            acc[0 : left.shape[0], :] += dot_nt(left, lane_hot)
        return total + forcing * residual

    total = lax.fori_loop(0, row_count // CHUNK, pack, jnp.zeros((1, CHUNK), F32))
    part = jnp.broadcast_to(0.5 * jnp.sum(total, axis=1, keepdims=True), (1, LANES))
    cost_send[...] = part
    for p in range(dev_count):
        for c in range(5):
            start = c * row_total + p * per_dest
            send[p, c * per_dest : (c + 1) * per_dest, :] = acc[start : start + per_dest, :]

    pl.semaphore_wait(barrier, len(partners))

    def data_copy(j):
        peer = peer_of(j)
        return pltpu.make_async_remote_copy(
            src_ref=send.at[peer], dst_ref=recv.at[j],
            send_sem=send_sem.at[j], recv_sem=recv_sem.at[j],
            device_id=(g, peer), device_id_type=MESH,
        )

    def cost_copy(j):
        return pltpu.make_async_remote_copy(
            src_ref=cost_send, dst_ref=cost_recv.at[j],
            send_sem=cost_send_sem.at[j], recv_sem=cost_recv_sem.at[j],
            device_id=(g, peer_of(j)), device_id_type=MESH,
        )

    def group_copy(j):
        return pltpu.make_async_remote_copy(
            src_ref=group_send, dst_ref=group_recv.at[j],
            send_sem=group_send_sem.at[j], recv_sem=group_recv_sem.at[j],
            device_id=wrapped(j, 0), device_id_type=MESH,
        )

    for j in range(1, dev_count):
        cost_copy(j).start()
    for j in range(1, dev_count):
        data_copy(j).start()
    recv[0] = send[d]

    raw[...] = jnp.zeros_like(raw)

    def element_sums(k, carry):
        for i in range(per_chunk):
            @pl.when(k * per_chunk + i > 0)
            def _():
                data_copy(k * per_chunk + i).wait_recv()

        def channel(c):
            rows = [
                recv[k * per_chunk + i, c * per_dest : (c + 1) * per_dest, :]
                for i in range(per_chunk)
            ]
            return rows[0] if per_chunk == 1 else jnp.concatenate(rows, axis=0)

        first_w = basis_values(channel(0))
        second_w = basis_values(channel(1))
        third_w = basis_values(channel(2))
        forcing = channel(3)
        owner = channel(4).astype(jnp.int32)
        for a in range(8):
            weighted = first_w[a] * forcing
            third[a] = third_w[a]
            for b in range(8):
                outer[a * 8 + b] = weighted * second_w[b]
        ids = lax.broadcasted_iota(jnp.int32, (ELEM_DEV, LANES), 0)
        for h in range(8):
            lanes = slice(h * LANES, (h + 1) * LANES)
            product = (outer[:, h : h + 1, :] * third[:, h, :][None]).reshape(512, LANES)
            rounded = product.astype(BF16)
            p_high[:, lanes] = rounded
            p_low[:, lanes] = (product - rounded.astype(F32)).astype(BF16)
            onehot[:, lanes] = jnp.where(
                ids == jnp.broadcast_to(owner[h : h + 1, :], (ELEM_DEV, LANES)), 1.0, 0.0
            ).astype(BF16)
        raw[...] += dot_nt(p_high[...], onehot[...]) + dot_nt(p_low[...], onehot[...])
        return carry

    chunk_count = dev_count // per_chunk
    middle = chunk_count // 2
    lax.fori_loop(0, middle, element_sums, 0)

    group_cost = cost_send[...]
    for j in range(1, dev_count):
        cost_copy(j).wait_recv()
        group_cost = group_cost + cost_recv[j]
    group_send[...] = group_cost
    for j in range(1, grp_count):
        group_copy(j).start()

    lax.fori_loop(middle, chunk_count, element_sums, 0)

    lane = lax.broadcasted_iota(jnp.int32, (1, LANES), 1)
    lower_half = lane < 64
    node = (lane // 8) % 8
    block = raw[448:512, 128:256]
    a_send[0] = jnp.where(lower_half, pltpu.roll(block[0:32], 64, 1), block[32:64])
    block = raw[0:64, 0:128]
    a_send[1] = jnp.where(lower_half, block[0:32], pltpu.roll(block[32:64], 64, 1))
    for half in range(2):
        columns = slice(half * LANES, (half + 1) * LANES)
        up = pltpu.roll(raw[56:64, columns], 72, 1)
        down = raw[0:8, columns]
        for a in range(1, 8):
            high = raw[a * 64 + 56 : a * 64 + 64, columns]
            low = raw[a * 64 : a * 64 + 8, columns]
            up = jnp.where(node == a, pltpu.roll(high, (a * 8 + 72) % 128, 1), up)
            down = jnp.where(node == a, pltpu.roll(low, a * 8, 1), down)
        b_send[0, half] = up
        b_send[1, half] = down

    steps = (1, -1)

    def face_copy(i):
        if i < 2:
            source, sink, target = a_send.at[i], a_recv.at[i], wrapped(steps[i], 0)
        else:
            source, sink, target = b_send.at[i - 2], b_recv.at[i - 2], wrapped(0, steps[i - 2])
        return pltpu.make_async_remote_copy(
            src_ref=source, dst_ref=sink,
            send_sem=face_send_sem.at[i], recv_sem=face_recv_sem.at[i],
            device_id=target, device_id_type=MESH,
        )

    def edge_copy(i, j):
        return pltpu.make_async_remote_copy(
            src_ref=b_send.at[j, 1 - i], dst_ref=edge_recv.at[j, i],
            send_sem=edge_send_sem.at[j, i], recv_sem=edge_recv_sem.at[j, i],
            device_id=wrapped(steps[i], steps[j]), device_id_type=MESH,
        )

    sends_a, sends_b = (g < grp_count - 1, g > 0), (d < dev_count - 1, d > 0)
    gets_a, gets_b = (g > 0, g < grp_count - 1), (d > 0, d < dev_count - 1)

    def when(condition, action):
        @pl.when(condition)
        def _():
            action()

    def clear(ref, i):
        ref[i] = jnp.zeros_like(ref[i])

    for j in range(2):
        for i in range(2):
            when(sends_a[i] & sends_b[j], lambda: edge_copy(i, j).start())
    for i in range(2):
        when(sends_a[i], lambda: face_copy(i).start())
        when(sends_b[i], lambda: face_copy(2 + i).start())

    for i in range(2):
        when(gets_a[i], lambda: face_copy(i).wait_recv())
        when(jnp.logical_not(gets_a[i]), lambda: clear(a_recv, i))
    low, high = raw[0:64, :], raw[448:512, :]
    from_low, from_high = a_recv[0], a_recv[1]
    from_low = jnp.concatenate([from_low, pltpu.roll(from_low, 64, 1)], axis=0)
    from_high = jnp.concatenate([pltpu.roll(from_high, 64, 1), from_high], axis=0)
    high_rolled = [pltpu.roll(high[:, :128], 64, 1), pltpu.roll(high[:, 128:], 64, 1)]
    low_rolled = [pltpu.roll(low[:, :128], 64, 1), pltpu.roll(low[:, 128:], 64, 1)]
    raw[0:64, 0:128] = low[:, :128] + jnp.where(lower_half, from_low, high_rolled[0])
    raw[0:64, 128:256] = low[:, 128:] + jnp.where(lower_half, high_rolled[0], high_rolled[1])
    raw[448:512, 0:128] = high[:, :128] + jnp.where(lower_half, low_rolled[0], low_rolled[1])
    raw[448:512, 128:256] = high[:, 128:] + jnp.where(lower_half, low_rolled[1], from_high)

    faces = []
    for j in range(2):
        when(gets_b[j], lambda: face_copy(2 + j).wait_recv())
        when(jnp.logical_not(gets_b[j]), lambda: clear(b_recv, j))
        for i in range(2):
            both = gets_a[i] & gets_b[j]
            when(both, lambda: edge_copy(i, j).wait_recv())
            when(jnp.logical_not(both), lambda: clear(edge_recv, (j, i)))
        first, second = b_recv[j, 0], b_recv[j, 1]
        up = [pltpu.roll(x, 8, 1) for x in (edge_recv[j, 0], first, second)]
        down = [pltpu.roll(x, 120, 1) for x in (first, second, edge_recv[j, 1])]
        face = []
        for half, own in enumerate((first, second)):
            from_low = jnp.where(lower_half, up[half], up[half + 1])
            from_high = jnp.where(lower_half, down[half], down[half + 1])
            face.append(
                own + jnp.where(node == 0, from_low, jnp.where(node == 7, from_high, 0.0))
            )
        faces.append(face)
    for half in range(2):
        columns = slice(half * LANES, (half + 1) * LANES)
        for a in range(8):
            low_rows = slice(a * 64, a * 64 + 8)
            high_rows = slice(a * 64 + 56, a * 64 + 64)
            low, high = raw[low_rows, columns], raw[high_rows, columns]
            got_low = pltpu.roll(faces[0][half], (128 - a * 8) % 128, 1)
            got_high = pltpu.roll(faces[1][half], (56 - a * 8) % 128, 1)
            raw[low_rows, columns] = low + jnp.where(node == 0, got_low, pltpu.roll(high, 8, 1))
            raw[high_rows, columns] = high + jnp.where(node == 7, got_high, pltpu.roll(low, 120, 1))

    ez = lax.broadcasted_iota(jnp.int32, (1, 8, LANES), 2) % 8
    c = lax.broadcasted_iota(jnp.int32, (1, 8, LANES), 1)
    takes_low = (c == 0) & (ez > 0)
    takes_high = (c == 7) & (ez < 7)
    for half in range(2):
        for part in range(4):
            rows = slice(part * 128, (part + 1) * 128)
            field = raw[rows, half * LANES : (half + 1) * LANES].reshape(16, 8, LANES)
            below = pltpu.roll(pltpu.roll(field, 1, 2), 1, 1)
            above = pltpu.roll(pltpu.roll(field, 127, 2), 7, 1)
            field = field + jnp.where(takes_low, below, jnp.where(takes_high, above, 0.0))
            out[half * LANES : (half + 1) * LANES, rows] = field.reshape(128, LANES).T

    all_cost = group_send[...]
    for j in range(1, grp_count):
        group_copy(j).wait_recv()
        all_cost = all_cost + group_recv[j]
    cost[...] = all_cost

    for j in range(1, dev_count):
        data_copy(j).wait_send()
        cost_copy(j).wait_send()
    for j in range(1, grp_count):
        group_copy(j).wait_send()
    for i in range(2):
        when(sends_a[i], lambda: face_copy(i).wait_send())
        when(sends_b[i], lambda: face_copy(2 + i).wait_send())
        for j in range(2):
            when(sends_a[i] & sends_b[j], lambda: edge_copy(i, j).wait_send())


def on_device(obs_coord, obs_resid, obs_weight, obs_dest, obs_send_slot, obs_elem, obs_slot):
    dev_count = lax.axis_size("dev")
    grp_count = lax.axis_size("grp")
    row_count = obs_resid.shape[0]
    capacity = 2 * row_count // dev_count
    per_dest = capacity // LANES
    vmem = pl.BlockSpec(memory_space=pltpu.VMEM)
    dma = pltpu.SemaphoreType.DMA
    rows = [x.reshape(1, row_count) for x in (obs_resid, obs_weight, obs_dest, obs_send_slot, obs_elem)]
    field, cost = pl.pallas_call(
        functools.partial(kernel, dev_count, grp_count, capacity),
        out_shape=(
            pltpu.VMEM((ELEM_DEV, 512), F32),
            pltpu.VMEM((1, LANES), F32),
        ),
        in_specs=[pl.BlockSpec(memory_space=pl.ANY)] * 6,
        out_specs=(vmem, vmem),
        scratch_shapes=[
            pltpu.VMEM((3, row_count), F32),
            pltpu.VMEM((1, row_count), F32),
            pltpu.VMEM((1, row_count), F32),
            pltpu.VMEM((1, row_count), jnp.int32),
            pltpu.VMEM((1, row_count), jnp.int32),
            pltpu.VMEM((1, row_count), jnp.int32),
            pltpu.VMEM((5 * 2 * row_count // LANES, LANES), F32),
            pltpu.VMEM((dev_count, 5 * per_dest, LANES), F32),
            pltpu.VMEM((dev_count, 5 * per_dest, LANES), F32),
            pltpu.VMEM((1, LANES), F32),
            pltpu.VMEM((dev_count, 1, LANES), F32),
            pltpu.VMEM((1, LANES), F32),
            pltpu.VMEM((grp_count, 1, LANES), F32),
            pltpu.VMEM((8, 8, LANES), F32),
            pltpu.VMEM((64, 8, LANES), F32),
            pltpu.VMEM((512, CHUNK), BF16),
            pltpu.VMEM((512, CHUNK), BF16),
            pltpu.VMEM((ELEM_DEV, CHUNK), BF16),
            pltpu.VMEM((512, ELEM_DEV), F32),
            pltpu.VMEM((2, 32, LANES), F32),
            pltpu.VMEM((2, 32, LANES), F32),
            pltpu.VMEM((2, 2, 8, LANES), F32),
            pltpu.VMEM((2, 2, 8, LANES), F32),
            dma((dev_count,)),
            dma((dev_count,)),
            dma((dev_count,)),
            dma((dev_count,)),
            dma((grp_count,)),
            dma((grp_count,)),
            dma((4,)),
            dma((4,)),
            pltpu.VMEM((2, 2, 8, LANES), F32),
            dma((2, 2)),
            dma((2, 2)),
            dma((6,)),
        ],
        compiler_params=pltpu.CompilerParams(collective_id=0, has_side_effects=True),
    )(obs_coord, *rows)
    return field.reshape(EX, EY, EZ, 512), cost[0, 0]


def solution(mesh):
    placed = (
        P(None, ("grp", "dev")),
        P(("grp", "dev")),
        P(("grp", "dev")),
        P(("grp", "dev")),
        P(("grp", "dev")),
        P(("grp", "dev")),
        P(("grp", "dev")),
    )
    return jax.shard_map(
        on_device,
        mesh=mesh,
        in_specs=placed,
        out_specs=(P("grp", "dev", None, None), P()),
        check_vma=False,
    )
```

```python
import functools
import math

import jax
import jax.numpy as jnp
from jax import lax
from jax.experimental import pallas as pl
from jax.experimental.pallas import tpu as pltpu
from jax.sharding import PartitionSpec as P

EX = 4
EY = 8
EZ = 8
ELEM_DEV = 256
LANES = 128
CHUNK = 1024
MESH = pl.DeviceIdType.MESH
F32 = jnp.float32
BF16 = jnp.bfloat16

ANCHORS = [-math.cos(math.pi * k / 7) for k in range(8)]
OUTER_PAIRS = [(a, b) for a in (0, 7) for b in range(8)]
OUTER_PAIRS += [(a, b) for a in range(1, 7) for b in (0, 7)]
INNER_PAIRS = [(a, b) for a in range(1, 7) for b in range(1, 7)]
PAIRS = OUTER_PAIRS + INNER_PAIRS
COEFS = [
    1.0 / math.prod(ANCHORS[a] - ANCHORS[m] for m in range(8) if m != a) for a in range(8)
]


def basis_values(t):
    factors = [t - p for p in ANCHORS]
    prefix = [None] * 8
    suffix = [None] * 8
    for k in range(1, 8):
        prefix[k] = factors[k - 1] if k == 1 else prefix[k - 1] * factors[k - 1]
    for k in range(6, -1, -1):
        suffix[k] = factors[k + 1] if k == 6 else suffix[k + 1] * factors[k + 1]
    basis = []
    for a in range(8):
        if a == 0:
            product = suffix[0]
        elif a == 7:
            product = prefix[7]
        else:
            product = prefix[a] * suffix[a]
        basis.append(product * COEFS[a])
    return basis


def dot_nt(left, right):
    return lax.dot_general(left, right, (((1,), (1,)), ((), ())), preferred_element_type=F32)


def split3(value):
    first = value.astype(BF16).astype(F32)
    rest = value - first
    second = rest.astype(BF16).astype(F32)
    return first, second, rest - second


def kernel(
    dev_count, grp_count, capacity,
    coord_in, resid_in, weight_in, dest_in, slot_in, elem_in,
    out, cost,
    coord, resid, weight, dest, slot, elem, acc, send, recv, cost_send, cost_recv, group_send, group_recv,
    third, outer, p_high, p_low, onehot, raw, a_send, a_recv, b_send, b_recv,
    send_sem, recv_sem, cost_send_sem, cost_recv_sem, group_send_sem, group_recv_sem,
    face_send_sem, face_recv_sem, edge_recv, edge_send_sem, edge_recv_sem, load_sem,
    face_rows, inner_rows,
):
    g = lax.axis_index("grp")
    d = lax.axis_index("dev")
    row_count = resid.shape[1]
    row_total = 2 * row_count // LANES
    per_dest = capacity // LANES
    per_chunk = 8 // per_dest

    def peer_of(k):
        peer, bit = 0, 1
        while bit < dev_count:
            peer = peer + lax.rem(d // bit + k // bit, 2) * bit
            bit *= 2
        return peer

    def wrapped(step_g, step_d):
        return (
            lax.rem(g + step_g + grp_count, grp_count),
            lax.rem(d + step_d + dev_count, dev_count),
        )

    barrier = pltpu.get_barrier_semaphore()
    partners = [(g, peer_of(k)) for k in range(1, dev_count)]
    partners += [wrapped(j, 0) for j in range(1, grp_count)]
    partners += [wrapped(i, j) for i in (-1, 1) for j in (-1, 1)]
    for partner in partners:
        pl.semaphore_signal(barrier, inc=1, device_id=partner, device_id_type=MESH)

    loads = [
        pltpu.make_async_copy(source, sink, load_sem.at[i])
        for i, (source, sink) in enumerate(
            zip(
                (dest_in, slot_in, resid_in, weight_in, coord_in, elem_in),
                (dest, slot, resid, weight, coord, elem),
            )
        )
    ]
    for load in loads:
        load.start()
    for load in loads:
        load.wait()

    acc[...] = jnp.zeros_like(acc)

    def pack(k, total):
        columns = pl.ds(pl.multiple_of(k * CHUNK, CHUNK), CHUNK)
        target = dest[:, columns] * capacity + slot[:, columns]
        high = jnp.broadcast_to(target // LANES, (row_total, CHUNK))
        low = jnp.broadcast_to(target % LANES, (LANES, CHUNK))
        row_hot = jnp.where(
            lax.broadcasted_iota(jnp.int32, (row_total, CHUNK), 0) == high, 1.0, 0.0
        ).astype(BF16)
        lane_hot = jnp.where(
            lax.broadcasted_iota(jnp.int32, (LANES, CHUNK), 0) == low, 1.0, 0.0
        ).astype(BF16)
        residual = resid[:, columns]
        forcing = weight[:, columns] * residual
        values = [coord[c : c + 1, columns] for c in range(3)] + [forcing]
        terms = [split3(value) for value in values]

        def spread(row):
            tile = jnp.broadcast_to(row, (16, CHUNK)).astype(BF16)
            return [row_hot[16 * i : 16 * i + 16] * tile for i in range(row_total // 16)]

        for t in range(3):
            pieces = []
            for channel in range(4):
                pieces += spread(terms[channel][t])
            if t == 0:
                pieces += spread(elem[:, columns].astype(F32))
            left = jnp.concatenate(pieces, axis=0)
            acc[0 : left.shape[0], :] += dot_nt(left, lane_hot)
        return total + forcing * residual

    total = lax.fori_loop(0, row_count // CHUNK, pack, jnp.zeros((1, CHUNK), F32))
    part = jnp.broadcast_to(0.5 * jnp.sum(total, axis=1, keepdims=True), (1, LANES))
    cost_send[...] = part
    for p in range(dev_count):
        for c in range(5):
            start = c * row_total + p * per_dest
            send[p, c * per_dest : (c + 1) * per_dest, :] = acc[start : start + per_dest, :]

    pl.semaphore_wait(barrier, len(partners))

    def data_copy(j):
        peer = peer_of(j)
        return pltpu.make_async_remote_copy(
            src_ref=send.at[peer], dst_ref=recv.at[j],
            send_sem=send_sem.at[j], recv_sem=recv_sem.at[j],
            device_id=(g, peer), device_id_type=MESH,
        )

    def cost_copy(j):
        return pltpu.make_async_remote_copy(
            src_ref=cost_send, dst_ref=cost_recv.at[j],
            send_sem=cost_send_sem.at[j], recv_sem=cost_recv_sem.at[j],
            device_id=(g, peer_of(j)), device_id_type=MESH,
        )

    def group_copy(j):
        return pltpu.make_async_remote_copy(
            src_ref=group_send, dst_ref=group_recv.at[j],
            send_sem=group_send_sem.at[j], recv_sem=group_recv_sem.at[j],
            device_id=wrapped(j, 0), device_id_type=MESH,
        )

    for j in range(1, dev_count):
        cost_copy(j).start()
    for j in range(1, dev_count):
        data_copy(j).start()
    recv[0] = send[d]

    face_rows[...] = jnp.zeros_like(face_rows)
    inner_rows[...] = jnp.zeros_like(inner_rows)

    def products(k, h, pairs):
        count = pairs.stop - pairs.start
        lanes = slice(h * LANES, (h + 1) * LANES)
        product = outer[k, pairs, h : h + 1, :] * third[k, :, h, :][None]
        product = product.reshape(count * 8, LANES)
        rounded = product.astype(BF16)
        p_high[0 : count * 8, lanes] = rounded
        p_low[0 : count * 8, lanes] = (product - rounded.astype(F32)).astype(BF16)

    def add_sums(k, sums):
        rows = slice(0, sums.shape[0])
        sums[...] += dot_nt(p_high[rows], onehot[k]) + dot_nt(p_low[rows], onehot[k])

    def element_sums(k, carry):
        for i in range(per_chunk):
            @pl.when(k * per_chunk + i > 0)
            def _():
                data_copy(k * per_chunk + i).wait_recv()

        def channel(c):
            rows = [
                recv[k * per_chunk + i, c * per_dest : (c + 1) * per_dest, :]
                for i in range(per_chunk)
            ]
            return rows[0] if per_chunk == 1 else jnp.concatenate(rows, axis=0)

        first_w = basis_values(channel(0))
        second_w = basis_values(channel(1))
        third_w = basis_values(channel(2))
        forcing = channel(3)
        owner = channel(4).astype(jnp.int32)
        weighted = [first * forcing for first in first_w]
        for c in range(8):
            third[k, c] = third_w[c]
        for i, (a, b) in enumerate(PAIRS):
            outer[k, i] = weighted[a] * second_w[b]
        ids = lax.broadcasted_iota(jnp.int32, (ELEM_DEV, LANES), 0)
        for h in range(8):
            products(k, h, slice(0, len(OUTER_PAIRS)))
            onehot[k, :, h * LANES : (h + 1) * LANES] = jnp.where(
                ids == jnp.broadcast_to(owner[h : h + 1, :], (ELEM_DEV, LANES)), 1.0, 0.0
            ).astype(BF16)
        add_sums(k, face_rows)
        return carry

    chunk_count = dev_count // per_chunk
    middle = chunk_count // 2
    lax.fori_loop(0, middle, element_sums, 0)

    group_cost = cost_send[...]
    for j in range(1, dev_count):
        cost_copy(j).wait_recv()
        group_cost = group_cost + cost_recv[j]
    group_send[...] = group_cost
    for j in range(1, grp_count):
        group_copy(j).start()

    lax.fori_loop(middle, chunk_count, element_sums, 0)

    def place(sums, pairs):
        for i, (a, b) in enumerate(pairs):
            start = a * 64 + b * 8
            raw[start : start + 8, :] = sums[i * 8 : i * 8 + 8, :]

    place(face_rows, OUTER_PAIRS)

    lane = lax.broadcasted_iota(jnp.int32, (1, LANES), 1)
    lower_half = lane < 64
    node = (lane // 8) % 8
    block = raw[448:512, 128:256]
    a_send[0] = jnp.where(lower_half, pltpu.roll(block[0:32], 64, 1), block[32:64])
    block = raw[0:64, 0:128]
    a_send[1] = jnp.where(lower_half, block[0:32], pltpu.roll(block[32:64], 64, 1))
    for half in range(2):
        columns = slice(half * LANES, (half + 1) * LANES)
        up = pltpu.roll(raw[56:64, columns], 72, 1)
        down = raw[0:8, columns]
        for a in range(1, 8):
            high = raw[a * 64 + 56 : a * 64 + 64, columns]
            low = raw[a * 64 : a * 64 + 8, columns]
            up = jnp.where(node == a, pltpu.roll(high, (a * 8 + 72) % 128, 1), up)
            down = jnp.where(node == a, pltpu.roll(low, a * 8, 1), down)
        b_send[0, half] = up
        b_send[1, half] = down

    steps = (1, -1)

    def face_copy(i):
        if i < 2:
            source, sink, target = a_send.at[i], a_recv.at[i], wrapped(steps[i], 0)
        else:
            source, sink, target = b_send.at[i - 2], b_recv.at[i - 2], wrapped(0, steps[i - 2])
        return pltpu.make_async_remote_copy(
            src_ref=source, dst_ref=sink,
            send_sem=face_send_sem.at[i], recv_sem=face_recv_sem.at[i],
            device_id=target, device_id_type=MESH,
        )

    def edge_copy(i, j):
        return pltpu.make_async_remote_copy(
            src_ref=b_send.at[j, 1 - i], dst_ref=edge_recv.at[j, i],
            send_sem=edge_send_sem.at[j, i], recv_sem=edge_recv_sem.at[j, i],
            device_id=wrapped(steps[i], steps[j]), device_id_type=MESH,
        )

    sends_a, sends_b = (g < grp_count - 1, g > 0), (d < dev_count - 1, d > 0)
    gets_a, gets_b = (g > 0, g < grp_count - 1), (d > 0, d < dev_count - 1)

    def when(condition, action):
        @pl.when(condition)
        def _():
            action()

    def clear(ref, i):
        ref[i] = jnp.zeros_like(ref[i])

    for j in range(2):
        for i in range(2):
            when(sends_a[i] & sends_b[j], lambda: edge_copy(i, j).start())
    for i in range(2):
        when(sends_a[i], lambda: face_copy(i).start())
        when(sends_b[i], lambda: face_copy(2 + i).start())

    def inner_sums(k, carry):
        for h in range(8):
            products(k, h, slice(len(OUTER_PAIRS), len(PAIRS)))
        add_sums(k, inner_rows)
        return carry

    lax.fori_loop(0, chunk_count, inner_sums, 0)
    place(inner_rows, INNER_PAIRS)

    for i in range(2):
        when(gets_a[i], lambda: face_copy(i).wait_recv())
        when(jnp.logical_not(gets_a[i]), lambda: clear(a_recv, i))
    low, high = raw[0:64, :], raw[448:512, :]
    from_low, from_high = a_recv[0], a_recv[1]
    from_low = jnp.concatenate([from_low, pltpu.roll(from_low, 64, 1)], axis=0)
    from_high = jnp.concatenate([pltpu.roll(from_high, 64, 1), from_high], axis=0)
    high_rolled = [pltpu.roll(high[:, :128], 64, 1), pltpu.roll(high[:, 128:], 64, 1)]
    low_rolled = [pltpu.roll(low[:, :128], 64, 1), pltpu.roll(low[:, 128:], 64, 1)]
    raw[0:64, 0:128] = low[:, :128] + jnp.where(lower_half, from_low, high_rolled[0])
    raw[0:64, 128:256] = low[:, 128:] + jnp.where(lower_half, high_rolled[0], high_rolled[1])
    raw[448:512, 0:128] = high[:, :128] + jnp.where(lower_half, low_rolled[0], low_rolled[1])
    raw[448:512, 128:256] = high[:, 128:] + jnp.where(lower_half, low_rolled[1], from_high)

    faces = []
    for j in range(2):
        when(gets_b[j], lambda: face_copy(2 + j).wait_recv())
        when(jnp.logical_not(gets_b[j]), lambda: clear(b_recv, j))
        for i in range(2):
            both = gets_a[i] & gets_b[j]
            when(both, lambda: edge_copy(i, j).wait_recv())
            when(jnp.logical_not(both), lambda: clear(edge_recv, (j, i)))
        first, second = b_recv[j, 0], b_recv[j, 1]
        up = [pltpu.roll(x, 8, 1) for x in (edge_recv[j, 0], first, second)]
        down = [pltpu.roll(x, 120, 1) for x in (first, second, edge_recv[j, 1])]
        face = []
        for half, own in enumerate((first, second)):
            from_low = jnp.where(lower_half, up[half], up[half + 1])
            from_high = jnp.where(lower_half, down[half], down[half + 1])
            face.append(
                own + jnp.where(node == 0, from_low, jnp.where(node == 7, from_high, 0.0))
            )
        faces.append(face)
    for half in range(2):
        columns = slice(half * LANES, (half + 1) * LANES)
        for a in range(8):
            low_rows = slice(a * 64, a * 64 + 8)
            high_rows = slice(a * 64 + 56, a * 64 + 64)
            low, high = raw[low_rows, columns], raw[high_rows, columns]
            got_low = pltpu.roll(faces[0][half], (128 - a * 8) % 128, 1)
            got_high = pltpu.roll(faces[1][half], (56 - a * 8) % 128, 1)
            raw[low_rows, columns] = low + jnp.where(node == 0, got_low, pltpu.roll(high, 8, 1))
            raw[high_rows, columns] = high + jnp.where(node == 7, got_high, pltpu.roll(low, 120, 1))

    ez = lax.broadcasted_iota(jnp.int32, (1, 8, LANES), 2) % 8
    c = lax.broadcasted_iota(jnp.int32, (1, 8, LANES), 1)
    takes_low = (c == 0) & (ez > 0)
    takes_high = (c == 7) & (ez < 7)
    for half in range(2):
        for part in range(4):
            rows = slice(part * 128, (part + 1) * 128)
            field = raw[rows, half * LANES : (half + 1) * LANES].reshape(16, 8, LANES)
            below = pltpu.roll(pltpu.roll(field, 1, 2), 1, 1)
            above = pltpu.roll(pltpu.roll(field, 127, 2), 7, 1)
            field = field + jnp.where(takes_low, below, jnp.where(takes_high, above, 0.0))
            out[half * LANES : (half + 1) * LANES, rows] = field.reshape(128, LANES).T

    all_cost = group_send[...]
    for j in range(1, grp_count):
        group_copy(j).wait_recv()
        all_cost = all_cost + group_recv[j]
    cost[...] = all_cost

    for j in range(1, dev_count):
        data_copy(j).wait_send()
        cost_copy(j).wait_send()
    for j in range(1, grp_count):
        group_copy(j).wait_send()
    for i in range(2):
        when(sends_a[i], lambda: face_copy(i).wait_send())
        when(sends_b[i], lambda: face_copy(2 + i).wait_send())
        for j in range(2):
            when(sends_a[i] & sends_b[j], lambda: edge_copy(i, j).wait_send())


def on_device(obs_coord, obs_resid, obs_weight, obs_dest, obs_send_slot, obs_elem, obs_slot):
    dev_count = lax.axis_size("dev")
    grp_count = lax.axis_size("grp")
    row_count = obs_resid.shape[0]
    capacity = 2 * row_count // dev_count
    per_dest = capacity // LANES
    chunks = 2 * row_count // CHUNK
    vmem = pl.BlockSpec(memory_space=pltpu.VMEM)
    dma = pltpu.SemaphoreType.DMA
    rows = [x.reshape(1, row_count) for x in (obs_resid, obs_weight, obs_dest, obs_send_slot, obs_elem)]
    field, cost = pl.pallas_call(
        functools.partial(kernel, dev_count, grp_count, capacity),
        out_shape=(
            pltpu.VMEM((ELEM_DEV, 512), F32),
            pltpu.VMEM((1, LANES), F32),
        ),
        in_specs=[pl.BlockSpec(memory_space=pl.ANY)] * 6,
        out_specs=(vmem, vmem),
        scratch_shapes=[
            pltpu.VMEM((3, row_count), F32),
            pltpu.VMEM((1, row_count), F32),
            pltpu.VMEM((1, row_count), F32),
            pltpu.VMEM((1, row_count), jnp.int32),
            pltpu.VMEM((1, row_count), jnp.int32),
            pltpu.VMEM((1, row_count), jnp.int32),
            pltpu.VMEM((5 * 2 * row_count // LANES, LANES), F32),
            pltpu.VMEM((dev_count, 5 * per_dest, LANES), F32),
            pltpu.VMEM((dev_count, 5 * per_dest, LANES), F32),
            pltpu.VMEM((1, LANES), F32),
            pltpu.VMEM((dev_count, 1, LANES), F32),
            pltpu.VMEM((1, LANES), F32),
            pltpu.VMEM((grp_count, 1, LANES), F32),
            pltpu.VMEM((chunks, 8, 8, LANES), F32),
            pltpu.VMEM((chunks, 64, 8, LANES), F32),
            pltpu.VMEM((len(INNER_PAIRS) * 8, CHUNK), BF16),
            pltpu.VMEM((len(INNER_PAIRS) * 8, CHUNK), BF16),
            pltpu.VMEM((chunks, ELEM_DEV, CHUNK), BF16),
            pltpu.VMEM((512, ELEM_DEV), F32),
            pltpu.VMEM((2, 32, LANES), F32),
            pltpu.VMEM((2, 32, LANES), F32),
            pltpu.VMEM((2, 2, 8, LANES), F32),
            pltpu.VMEM((2, 2, 8, LANES), F32),
            dma((dev_count,)),
            dma((dev_count,)),
            dma((dev_count,)),
            dma((dev_count,)),
            dma((grp_count,)),
            dma((grp_count,)),
            dma((4,)),
            dma((4,)),
            pltpu.VMEM((2, 2, 8, LANES), F32),
            dma((2, 2)),
            dma((2, 2)),
            dma((6,)),
            pltpu.VMEM((len(OUTER_PAIRS) * 8, ELEM_DEV), F32),
            pltpu.VMEM((len(INNER_PAIRS) * 8, ELEM_DEV), F32),
        ],
        compiler_params=pltpu.CompilerParams(collective_id=0, has_side_effects=True),
    )(obs_coord, *rows)
    return field.reshape(EX, EY, EZ, 512), cost[0, 0]


def solution(mesh):
    placed = (
        P(None, ("grp", "dev")),
        P(("grp", "dev")),
        P(("grp", "dev")),
        P(("grp", "dev")),
        P(("grp", "dev")),
        P(("grp", "dev")),
        P(("grp", "dev")),
    )
    return jax.shard_map(
        on_device,
        mesh=mesh,
        in_specs=placed,
        out_specs=(P("grp", "dev", None, None), P()),
        check_vma=False,
    )
```

```python
import functools
import math

import jax
import jax.numpy as jnp
from jax import lax
from jax.experimental import pallas as pl
from jax.experimental.pallas import tpu as pltpu
from jax.sharding import PartitionSpec as P

EX = 4
EY = 8
EZ = 8
ELEM_DEV = 256
LANES = 128
CHUNK = 1024
MESH = pl.DeviceIdType.MESH
F32 = jnp.float32
BF16 = jnp.bfloat16

ANCHORS = [-math.cos(math.pi * k / 7) for k in range(8)]
OUTER_PAIRS = [(a, b) for a in (0, 7) for b in range(8)]
OUTER_PAIRS += [(a, b) for a in range(1, 7) for b in (0, 7)]
INNER_PAIRS = [(a, b) for a in range(1, 7) for b in range(1, 7)]
PAIRS = OUTER_PAIRS + INNER_PAIRS
COEFS = [
    1.0 / math.prod(ANCHORS[a] - ANCHORS[m] for m in range(8) if m != a) for a in range(8)
]


def basis_values(t):
    factors = [t - p for p in ANCHORS]
    prefix = [None] * 8
    suffix = [None] * 8
    for k in range(1, 8):
        prefix[k] = factors[k - 1] if k == 1 else prefix[k - 1] * factors[k - 1]
    for k in range(6, -1, -1):
        suffix[k] = factors[k + 1] if k == 6 else suffix[k + 1] * factors[k + 1]
    basis = []
    for a in range(8):
        if a == 0:
            product = suffix[0]
        elif a == 7:
            product = prefix[7]
        else:
            product = prefix[a] * suffix[a]
        basis.append(product * COEFS[a])
    return basis


def dot_nt(left, right):
    return lax.dot_general(left, right, (((1,), (1,)), ((), ())), preferred_element_type=F32)


def split3(value):
    first = value.astype(BF16).astype(F32)
    rest = value - first
    second = rest.astype(BF16).astype(F32)
    return first, second, rest - second


def kernel(
    dev_count, grp_count, capacity,
    coord_in, resid_in, weight_in, dest_in, slot_in, elem_in,
    out, cost,
    coord, resid, weight, dest, slot, elem, acc, send, recv, cost_send, cost_recv, group_send, group_recv,
    third, outer, p_high, p_low, onehot, raw, a_send, a_recv, b_send, b_recv,
    send_sem, recv_sem, cost_send_sem, cost_recv_sem, group_send_sem, group_recv_sem,
    face_send_sem, face_recv_sem, edge_recv, edge_send_sem, edge_recv_sem, load_sem,
    face_rows, inner_rows,
):
    g = lax.axis_index("grp")
    d = lax.axis_index("dev")
    row_count = resid.shape[1]
    row_total = 2 * row_count // LANES
    per_dest = capacity // LANES
    per_chunk = 8 // per_dest

    def peer_of(k):
        peer, bit = 0, 1
        while bit < dev_count:
            peer = peer + lax.rem(d // bit + k // bit, 2) * bit
            bit *= 2
        return peer

    def wrapped(step_g, step_d):
        return (
            lax.rem(g + step_g + grp_count, grp_count),
            lax.rem(d + step_d + dev_count, dev_count),
        )

    barrier = pltpu.get_barrier_semaphore()
    partners = [(g, peer_of(k)) for k in range(1, dev_count)]
    partners += [wrapped(j, 0) for j in range(1, grp_count)]
    partners += [wrapped(i, j) for i in (-1, 1) for j in (-1, 1)]
    for partner in partners:
        pl.semaphore_signal(barrier, inc=1, device_id=partner, device_id_type=MESH)

    loads = [
        pltpu.make_async_copy(source, sink, load_sem.at[i])
        for i, (source, sink) in enumerate(
            zip(
                (dest_in, slot_in, resid_in, weight_in, coord_in, elem_in),
                (dest, slot, resid, weight, coord, elem),
            )
        )
    ]
    for load in loads:
        load.start()
    for load in loads:
        load.wait()

    acc[...] = jnp.zeros_like(acc)

    def pack(k, total):
        columns = pl.ds(pl.multiple_of(k * CHUNK, CHUNK), CHUNK)
        target = dest[:, columns] * capacity + slot[:, columns]
        high = jnp.broadcast_to(target // LANES, (row_total, CHUNK))
        low = jnp.broadcast_to(target % LANES, (LANES, CHUNK))
        row_hot = jnp.where(
            lax.broadcasted_iota(jnp.int32, (row_total, CHUNK), 0) == high, 1.0, 0.0
        ).astype(BF16)
        lane_hot = jnp.where(
            lax.broadcasted_iota(jnp.int32, (LANES, CHUNK), 0) == low, 1.0, 0.0
        ).astype(BF16)
        residual = resid[:, columns]
        forcing = weight[:, columns] * residual
        values = [coord[c : c + 1, columns] for c in range(3)] + [forcing]
        terms = [split3(value) for value in values]

        def spread(row):
            tile = jnp.broadcast_to(row, (16, CHUNK)).astype(BF16)
            return [row_hot[16 * i : 16 * i + 16] * tile for i in range(row_total // 16)]

        for t in range(3):
            pieces = []
            for channel in range(4):
                pieces += spread(terms[channel][t])
            if t == 0:
                pieces += spread(elem[:, columns].astype(F32))
            left = jnp.concatenate(pieces, axis=0)
            acc[0 : left.shape[0], :] += dot_nt(left, lane_hot)
        return total + forcing * residual

    total = lax.fori_loop(0, row_count // CHUNK, pack, jnp.zeros((1, CHUNK), F32), unroll=True)
    part = jnp.broadcast_to(0.5 * jnp.sum(total, axis=1, keepdims=True), (1, LANES))
    cost_send[...] = part
    for p in range(dev_count):
        for c in range(5):
            start = c * row_total + p * per_dest
            send[p, c * per_dest : (c + 1) * per_dest, :] = acc[start : start + per_dest, :]

    pl.semaphore_wait(barrier, len(partners))

    def data_copy(j):
        peer = peer_of(j)
        return pltpu.make_async_remote_copy(
            src_ref=send.at[peer], dst_ref=recv.at[j],
            send_sem=send_sem.at[j], recv_sem=recv_sem.at[j],
            device_id=(g, peer), device_id_type=MESH,
        )

    def cost_copy(j):
        return pltpu.make_async_remote_copy(
            src_ref=cost_send, dst_ref=cost_recv.at[j],
            send_sem=cost_send_sem.at[j], recv_sem=cost_recv_sem.at[j],
            device_id=(g, peer_of(j)), device_id_type=MESH,
        )

    def group_copy(j):
        return pltpu.make_async_remote_copy(
            src_ref=group_send, dst_ref=group_recv.at[j],
            send_sem=group_send_sem.at[j], recv_sem=group_recv_sem.at[j],
            device_id=wrapped(j, 0), device_id_type=MESH,
        )

    for j in range(1, dev_count):
        cost_copy(j).start()
    for j in range(1, dev_count):
        data_copy(j).start()
    recv[0] = send[d]

    face_rows[...] = jnp.zeros_like(face_rows)
    inner_rows[...] = jnp.zeros_like(inner_rows)

    def products(k, h, pairs):
        count = pairs.stop - pairs.start
        lanes = slice(h * LANES, (h + 1) * LANES)
        product = outer[k, pairs, h : h + 1, :] * third[k, :, h, :][None]
        product = product.reshape(count * 8, LANES)
        rounded = product.astype(BF16)
        p_high[0 : count * 8, lanes] = rounded
        p_low[0 : count * 8, lanes] = (product - rounded.astype(F32)).astype(BF16)

    def add_sums(k, sums):
        rows = slice(0, sums.shape[0])
        sums[...] += dot_nt(p_high[rows], onehot[k]) + dot_nt(p_low[rows], onehot[k])

    def element_sums(k, carry):
        for i in range(per_chunk):
            @pl.when(k * per_chunk + i > 0)
            def _():
                data_copy(k * per_chunk + i).wait_recv()

        def channel(c):
            rows = [
                recv[k * per_chunk + i, c * per_dest : (c + 1) * per_dest, :]
                for i in range(per_chunk)
            ]
            return rows[0] if per_chunk == 1 else jnp.concatenate(rows, axis=0)

        first_w = basis_values(channel(0))
        second_w = basis_values(channel(1))
        third_w = basis_values(channel(2))
        forcing = channel(3)
        owner = channel(4).astype(jnp.int32)
        weighted = [first * forcing for first in first_w]
        for c in range(8):
            third[k, c] = third_w[c]
        for i, (a, b) in enumerate(PAIRS):
            outer[k, i] = weighted[a] * second_w[b]
        ids = lax.broadcasted_iota(jnp.int32, (ELEM_DEV, LANES), 0)
        for h in range(8):
            products(k, h, slice(0, len(OUTER_PAIRS)))
            onehot[k, :, h * LANES : (h + 1) * LANES] = jnp.where(
                ids == jnp.broadcast_to(owner[h : h + 1, :], (ELEM_DEV, LANES)), 1.0, 0.0
            ).astype(BF16)
        add_sums(k, face_rows)
        return carry

    chunk_count = dev_count // per_chunk
    lax.fori_loop(0, chunk_count, element_sums, 0)

    def place(sums, pairs):
        for i, (a, b) in enumerate(pairs):
            start = a * 64 + b * 8
            raw[start : start + 8, :] = sums[i * 8 : i * 8 + 8, :]

    place(face_rows, OUTER_PAIRS)

    lane = lax.broadcasted_iota(jnp.int32, (1, LANES), 1)
    lower_half = lane < 64
    node = (lane // 8) % 8
    block = raw[448:512, 128:256]
    a_send[0] = jnp.where(lower_half, pltpu.roll(block[0:32], 64, 1), block[32:64])
    block = raw[0:64, 0:128]
    a_send[1] = jnp.where(lower_half, block[0:32], pltpu.roll(block[32:64], 64, 1))
    for half in range(2):
        columns = slice(half * LANES, (half + 1) * LANES)
        up = pltpu.roll(raw[56:64, columns], 72, 1)
        down = raw[0:8, columns]
        for a in range(1, 8):
            high = raw[a * 64 + 56 : a * 64 + 64, columns]
            low = raw[a * 64 : a * 64 + 8, columns]
            up = jnp.where(node == a, pltpu.roll(high, (a * 8 + 72) % 128, 1), up)
            down = jnp.where(node == a, pltpu.roll(low, a * 8, 1), down)
        b_send[0, half] = up
        b_send[1, half] = down

    steps = (1, -1)

    def face_copy(i):
        if i < 2:
            source, sink, target = a_send.at[i], a_recv.at[i], wrapped(steps[i], 0)
        else:
            source, sink, target = b_send.at[i - 2], b_recv.at[i - 2], wrapped(0, steps[i - 2])
        return pltpu.make_async_remote_copy(
            src_ref=source, dst_ref=sink,
            send_sem=face_send_sem.at[i], recv_sem=face_recv_sem.at[i],
            device_id=target, device_id_type=MESH,
        )

    def edge_copy(i, j):
        return pltpu.make_async_remote_copy(
            src_ref=b_send.at[j, 1 - i], dst_ref=edge_recv.at[j, i],
            send_sem=edge_send_sem.at[j, i], recv_sem=edge_recv_sem.at[j, i],
            device_id=wrapped(steps[i], steps[j]), device_id_type=MESH,
        )

    sends_a, sends_b = (g < grp_count - 1, g > 0), (d < dev_count - 1, d > 0)
    gets_a, gets_b = (g > 0, g < grp_count - 1), (d > 0, d < dev_count - 1)

    def when(condition, action):
        @pl.when(condition)
        def _():
            action()

    def clear(ref, i):
        ref[i] = jnp.zeros_like(ref[i])

    for j in range(2):
        for i in range(2):
            when(sends_a[i] & sends_b[j], lambda: edge_copy(i, j).start())
    for i in range(2):
        when(sends_a[i], lambda: face_copy(i).start())
        when(sends_b[i], lambda: face_copy(2 + i).start())

    group_cost = cost_send[...]
    for j in range(1, dev_count):
        cost_copy(j).wait_recv()
        group_cost = group_cost + cost_recv[j]
    group_send[...] = group_cost
    for j in range(1, grp_count):
        group_copy(j).start()

    def inner_sums(k, carry):
        for h in range(8):
            products(k, h, slice(len(OUTER_PAIRS), len(PAIRS)))
        add_sums(k, inner_rows)
        return carry

    lax.fori_loop(0, chunk_count, inner_sums, 0)
    place(inner_rows, INNER_PAIRS)

    for i in range(2):
        when(gets_a[i], lambda: face_copy(i).wait_recv())
        when(jnp.logical_not(gets_a[i]), lambda: clear(a_recv, i))
    low, high = raw[0:64, :], raw[448:512, :]
    from_low, from_high = a_recv[0], a_recv[1]
    from_low = jnp.concatenate([from_low, pltpu.roll(from_low, 64, 1)], axis=0)
    from_high = jnp.concatenate([pltpu.roll(from_high, 64, 1), from_high], axis=0)
    high_rolled = [pltpu.roll(high[:, :128], 64, 1), pltpu.roll(high[:, 128:], 64, 1)]
    low_rolled = [pltpu.roll(low[:, :128], 64, 1), pltpu.roll(low[:, 128:], 64, 1)]
    raw[0:64, 0:128] = low[:, :128] + jnp.where(lower_half, from_low, high_rolled[0])
    raw[0:64, 128:256] = low[:, 128:] + jnp.where(lower_half, high_rolled[0], high_rolled[1])
    raw[448:512, 0:128] = high[:, :128] + jnp.where(lower_half, low_rolled[0], low_rolled[1])
    raw[448:512, 128:256] = high[:, 128:] + jnp.where(lower_half, low_rolled[1], from_high)

    faces = []
    for j in range(2):
        when(gets_b[j], lambda: face_copy(2 + j).wait_recv())
        when(jnp.logical_not(gets_b[j]), lambda: clear(b_recv, j))
        for i in range(2):
            both = gets_a[i] & gets_b[j]
            when(both, lambda: edge_copy(i, j).wait_recv())
            when(jnp.logical_not(both), lambda: clear(edge_recv, (j, i)))
        first, second = b_recv[j, 0], b_recv[j, 1]
        up = [pltpu.roll(x, 8, 1) for x in (edge_recv[j, 0], first, second)]
        down = [pltpu.roll(x, 120, 1) for x in (first, second, edge_recv[j, 1])]
        face = []
        for half, own in enumerate((first, second)):
            from_low = jnp.where(lower_half, up[half], up[half + 1])
            from_high = jnp.where(lower_half, down[half], down[half + 1])
            face.append(
                own + jnp.where(node == 0, from_low, jnp.where(node == 7, from_high, 0.0))
            )
        faces.append(face)
    for half in range(2):
        columns = slice(half * LANES, (half + 1) * LANES)
        for a in range(8):
            low_rows = slice(a * 64, a * 64 + 8)
            high_rows = slice(a * 64 + 56, a * 64 + 64)
            low, high = raw[low_rows, columns], raw[high_rows, columns]
            got_low = pltpu.roll(faces[0][half], (128 - a * 8) % 128, 1)
            got_high = pltpu.roll(faces[1][half], (56 - a * 8) % 128, 1)
            raw[low_rows, columns] = low + jnp.where(node == 0, got_low, pltpu.roll(high, 8, 1))
            raw[high_rows, columns] = high + jnp.where(node == 7, got_high, pltpu.roll(low, 120, 1))

    ez = lax.broadcasted_iota(jnp.int32, (1, 8, LANES), 2) % 8
    c = lax.broadcasted_iota(jnp.int32, (1, 8, LANES), 1)
    takes_low = (c == 0) & (ez > 0)
    takes_high = (c == 7) & (ez < 7)
    for half in range(2):
        for part in range(4):
            rows = slice(part * 128, (part + 1) * 128)
            field = raw[rows, half * LANES : (half + 1) * LANES].reshape(16, 8, LANES)
            below = pltpu.roll(pltpu.roll(field, 1, 2), 1, 1)
            above = pltpu.roll(pltpu.roll(field, 127, 2), 7, 1)
            field = field + jnp.where(takes_low, below, jnp.where(takes_high, above, 0.0))
            out[half * LANES : (half + 1) * LANES, rows] = field.reshape(128, LANES).T

    all_cost = group_send[...]
    for j in range(1, grp_count):
        group_copy(j).wait_recv()
        all_cost = all_cost + group_recv[j]
    cost[...] = all_cost

    for j in range(1, dev_count):
        data_copy(j).wait_send()
        cost_copy(j).wait_send()
    for j in range(1, grp_count):
        group_copy(j).wait_send()
    for i in range(2):
        when(sends_a[i], lambda: face_copy(i).wait_send())
        when(sends_b[i], lambda: face_copy(2 + i).wait_send())
        for j in range(2):
            when(sends_a[i] & sends_b[j], lambda: edge_copy(i, j).wait_send())


def on_device(obs_coord, obs_resid, obs_weight, obs_dest, obs_send_slot, obs_elem, obs_slot):
    dev_count = lax.axis_size("dev")
    grp_count = lax.axis_size("grp")
    row_count = obs_resid.shape[0]
    capacity = 2 * row_count // dev_count
    per_dest = capacity // LANES
    chunks = 2 * row_count // CHUNK
    vmem = pl.BlockSpec(memory_space=pltpu.VMEM)
    dma = pltpu.SemaphoreType.DMA
    rows = [x.reshape(1, row_count) for x in (obs_resid, obs_weight, obs_dest, obs_send_slot, obs_elem)]
    field, cost = pl.pallas_call(
        functools.partial(kernel, dev_count, grp_count, capacity),
        out_shape=(
            pltpu.VMEM((ELEM_DEV, 512), F32),
            pltpu.VMEM((1, LANES), F32),
        ),
        in_specs=[pl.BlockSpec(memory_space=pl.ANY)] * 6,
        out_specs=(vmem, vmem),
        scratch_shapes=[
            pltpu.VMEM((3, row_count), F32),
            pltpu.VMEM((1, row_count), F32),
            pltpu.VMEM((1, row_count), F32),
            pltpu.VMEM((1, row_count), jnp.int32),
            pltpu.VMEM((1, row_count), jnp.int32),
            pltpu.VMEM((1, row_count), jnp.int32),
            pltpu.VMEM((5 * 2 * row_count // LANES, LANES), F32),
            pltpu.VMEM((dev_count, 5 * per_dest, LANES), F32),
            pltpu.VMEM((dev_count, 5 * per_dest, LANES), F32),
            pltpu.VMEM((1, LANES), F32),
            pltpu.VMEM((dev_count, 1, LANES), F32),
            pltpu.VMEM((1, LANES), F32),
            pltpu.VMEM((grp_count, 1, LANES), F32),
            pltpu.VMEM((chunks, 8, 8, LANES), F32),
            pltpu.VMEM((chunks, 64, 8, LANES), F32),
            pltpu.VMEM((len(INNER_PAIRS) * 8, CHUNK), BF16),
            pltpu.VMEM((len(INNER_PAIRS) * 8, CHUNK), BF16),
            pltpu.VMEM((chunks, ELEM_DEV, CHUNK), BF16),
            pltpu.VMEM((512, ELEM_DEV), F32),
            pltpu.VMEM((2, 32, LANES), F32),
            pltpu.VMEM((2, 32, LANES), F32),
            pltpu.VMEM((2, 2, 8, LANES), F32),
            pltpu.VMEM((2, 2, 8, LANES), F32),
            dma((dev_count,)),
            dma((dev_count,)),
            dma((dev_count,)),
            dma((dev_count,)),
            dma((grp_count,)),
            dma((grp_count,)),
            dma((4,)),
            dma((4,)),
            pltpu.VMEM((2, 2, 8, LANES), F32),
            dma((2, 2)),
            dma((2, 2)),
            dma((6,)),
            pltpu.VMEM((len(OUTER_PAIRS) * 8, ELEM_DEV), F32),
            pltpu.VMEM((len(INNER_PAIRS) * 8, ELEM_DEV), F32),
        ],
        compiler_params=pltpu.CompilerParams(collective_id=0, has_side_effects=True),
    )(obs_coord, *rows)
    return field.reshape(EX, EY, EZ, 512), cost[0, 0]


def solution(mesh):
    placed = (
        P(None, ("grp", "dev")),
        P(("grp", "dev")),
        P(("grp", "dev")),
        P(("grp", "dev")),
        P(("grp", "dev")),
        P(("grp", "dev")),
        P(("grp", "dev")),
    )
    return jax.shard_map(
        on_device,
        mesh=mesh,
        in_specs=placed,
        out_specs=(P("grp", "dev", None, None), P()),
        check_vma=False,
    )
```
